32 devices in a mesh: slab: 4 (over x, core), patch: 8 (over z, y).
Axes of the slice: x: 2, y: 2, z: 4, core: 2. Of those that a mesh axis runs over, the one named last changes fastest.
Arguments:
- right_side: float32 [4, 8, 256, 768], P('slab', 'patch'), may hold values from -6 to 6
- inverse_factor: bfloat16 [4, 8, 768, 768], P('slab', 'patch'), may hold values from -0.12990381 to 1.5, as said below
- forward_trace: bfloat16 [4, 8, 128, 768], P('slab', 'patch'), may hold values from -0.375 to 0.375
- backward_trace: bfloat16 [4, 8, 128, 768], P('slab', 'patch'), may hold values from -0.375 to 0.375
- margin: int32 [4, 8], P('slab', 'patch'), may hold values from 1 to 256, as said below
Outputs:
- correction: float32 [4, 8, 256, 768], P('slab', 'patch')
The draws below stay inside these ranges and needn't reach their ends.
Inputs may be any that keep to these rules, and one draw needn't show every extreme that they name: `inverse_factor`: lower triangular: zero above the diagonal, positive on it. margin[s, q] counts the last unknowns of patch q that are the first unknowns of patch q + 1 (of patch 0 for q = 7). In every slab some pair shares exactly 256.
All inputs are finite; a program needn't handle non-finite values.
Results may differ from the reference program's by a relative error of at most 0.035.
Values may be sent and summed in bfloat16 or wider, within the bound.
A program may use at most 64 MiB of HBM per device.

```python
import math
import jax
import jax.numpy as jnp
from jax import lax

M = 768
KMAX = 256
FACE = 128
COLS = 256
SLABS = 4
PATCHES = 8


def draw_inverse_factor(key, part):
    first_key = jax.random.fold_in(key, 11)
    second_key = jax.random.fold_in(key, 12)
    full_shape = (SLABS, PATCHES, M, M)
    spread = jnp.clip(0.6 * jax.random.normal(first_key, full_shape, jnp.float32), -3.6, 3.6)
    diagonal = jax.random.uniform(second_key, (SLABS, PATCHES, M), jnp.float32, 0.7, 1.3)
    row_index = jnp.arange(M)[:, None]
    col_index = jnp.arange(M)[None, :]
    lower_part = jnp.where(row_index > col_index, spread, 0.0) / math.sqrt(M)
    matrix = lower_part + jnp.where(row_index == col_index, 1.0, 0.0) * diagonal[..., :, None]
    return matrix.astype(jnp.bfloat16)


def draw_margin(key, part):
    values = jax.random.randint(jax.random.fold_in(key, 21), (SLABS, PATCHES), 1, KMAX + 1)
    chosen = jax.random.randint(jax.random.fold_in(key, 22), (SLABS, 1), 0, PATCHES)
    return jnp.where(jnp.arange(PATCHES)[None, :] == chosen, KMAX, values).astype(jnp.int32)


def steps_of(key, shape, cuts, least, largest):
    level, own = 1.0, jax.random.fold_in(key, 6)
    for axis_at, shards_of in cuts:
        draws = jnp.exp(jax.random.uniform(jax.random.fold_in(own, axis_at), (shards_of,), jnp.float32, least / len(cuts), largest / len(cuts)))
        level = level * jnp.repeat(draws, shape[axis_at] // shards_of).reshape([-1 if axis == axis_at else 1 for axis in range(len(shape))])
    return level


def gaussian(stream_key, extent, width, bound, cuts=(), kind=jnp.bfloat16):
    drawn = jax.random.normal(stream_key, extent, jnp.float32) * width
    if len(cuts) > 0:
        drawn = steps_of(stream_key, extent, cuts, -0.22, 0.18) * drawn
    return jnp.clip(drawn, min=-bound, max=bound).astype(kind)


def setup_inputs(seed: int = 0) -> dict:
    keys = jax.random.split(jax.random.key(seed), 6)
    right_side = gaussian(keys[0], (SLABS, PATCHES, COLS, M), 1.0, 6.0, ((0, 4), (1, 8)), jnp.float32)
    inverse_factor = draw_inverse_factor(jax.random.fold_in(keys[5], 71), 0)
    forward_trace = gaussian(keys[2], (SLABS, PATCHES, FACE, M), (2 * FACE) ** -0.5, 0.375, ((0, 4), (1, 8)))
    backward_trace = gaussian(keys[3], (SLABS, PATCHES, FACE, M), (2 * FACE) ** -0.5, 0.375, ((0, 4), (1, 8)))
    margin = draw_margin(jax.random.fold_in(keys[5], 71), 0)
    return {"right_side": right_side, "inverse_factor": inverse_factor, "forward_trace": forward_trace, "backward_trace": backward_trace, "margin": margin}


def to_half(values):
    return lax.optimization_barrier(values.astype(jnp.bfloat16)).astype(jnp.float32)


def placement(counts):
    source_index = jnp.arange(KMAX, dtype=jnp.int32)[None, :, None]
    target_index = jnp.arange(KMAX, dtype=jnp.int32)[None, None, :]
    limit = counts.astype(jnp.int32)[:, None, None]
    hit = (source_index == KMAX - limit + target_index) & (target_index < limit)
    return jnp.where(hit, 1.0, 0.0).astype(jnp.float32)


def solve(values, factor):
    halfway = to_half(jnp.einsum('pck,pik->pci', to_half(values), factor))
    return jnp.einsum('pci,pik->pck', halfway, factor)


def slab_step(residual, factor, counts):
    initial = to_half(solve(residual, factor))
    placing = placement(counts)
    tail_rows = initial[:, :, M - KMAX:]
    head_rows = initial[:, :, :KMAX]
    from_left = jnp.roll(jnp.einsum('pcs,psd->pcd', tail_rows, placing), 1, axis=0)
    from_right = jnp.einsum('pci,pti->pct', jnp.roll(head_rows, -1, axis=0), placing)
    middle = jnp.zeros((residual.shape[0], residual.shape[1], M - 2 * KMAX), jnp.float32)
    shared = jnp.concatenate([from_left, middle, from_right], axis=2)
    return solve(residual - 0.5 * shared, factor)


def face_map(matrix, corrected):
    return to_half(jnp.einsum('pck,ptk->pct', to_half(corrected), matrix))


def face_terms(down_face, up_face):
    middle = jnp.zeros((down_face.shape[0], down_face.shape[1], M - 2 * FACE), jnp.float32)
    return jnp.concatenate([down_face, middle, up_face], axis=2)


def reference(right_side, inverse_factor, forward_trace, backward_trace, margin):
    zero_face = jnp.zeros((PATCHES, COLS, FACE), jnp.float32)
    down_store = []
    arriving = zero_face
    forward_last = None
    for slab_index in range(SLABS):
        factor = inverse_factor[slab_index].astype(jnp.float32)
        residual = right_side[slab_index] - face_terms(arriving, zero_face)
        corrected = slab_step(residual, factor, margin[slab_index])
        down_store.append(arriving)
        arriving = face_map(forward_trace[slab_index].astype(jnp.float32), corrected)
        forward_last = corrected
    results = [None] * SLABS
    up_face = zero_face
    for slab_index in range(SLABS - 1, -1, -1):
        factor = inverse_factor[slab_index].astype(jnp.float32)
        if slab_index == SLABS - 1:
            corrected = forward_last
        else:
            residual = right_side[slab_index] - face_terms(down_store[slab_index], up_face)
            corrected = slab_step(residual, factor, margin[slab_index])
        results[slab_index] = corrected
        up_face = face_map(backward_trace[slab_index].astype(jnp.float32), corrected)
    return jnp.stack(results, axis=0)
```

```python
import functools

import jax
import jax.numpy as jnp
from jax import lax
from jax.experimental import pallas as pl
from jax.experimental.pallas import tpu as pltpu
from jax.sharding import PartitionSpec as P

KMAX = 256
BF = jnp.bfloat16
F32 = jnp.float32
MESH = pl.DeviceIdType.MESH


def nt(a, b):
    return lax.dot_general(a, b, (((1,), (1,)), ((), ())), preferred_element_type=F32)


def nn(a, b):
    return lax.dot_general(a, b, (((1,), (0,)), ((), ())), preferred_element_type=F32)


def tn(a, b):
    return lax.dot_general(a, b, (((0,), (0,)), ((), ())), preferred_element_type=F32)


def solve(x, fac, m):
    half = jnp.concatenate(
        [nt(x[:, : i + KMAX], fac[i : i + KMAX, : i + KMAX]).astype(BF) for i in range(0, m, KMAX)],
        axis=1,
    )
    return [nn(half[:, k:], fac[k:, k : k + KMAX]) for k in range(0, m, KMAX)]


def kernel(
    slabs, patches,
    r_ref, l_ref, f_ref, b_ref, margin_ref, out_ref,
    tail_s, head_s, zt_s, zh_s, d_s, u_s,
    tail_r, head_r, zt_r, zh_r, d_r, u_r,
    adj, acc, gt, opd, opu, place, zr,
    send_sem, recv_sem,
):
    s = lax.axis_index("slab")
    q = lax.axis_index("patch")
    left = lax.rem(q + patches - 1, patches)
    right = lax.rem(q + 1, patches)
    around = (q, left, right)
    m = l_ref.shape[-1]
    face = f_ref.shape[-2]
    fac = l_ref.at[0, 0]

    barrier = pltpu.get_barrier_semaphore()

    def greet(slab, patch):
        pl.semaphore_signal(barrier, inc=1, device_id=(slab, patch), device_id_type=MESH)

    greet(s, left)
    greet(s, right)

    @pl.when(s > 0)
    def _():
        for p in around:
            greet(s - 1, p)

    @pl.when(s < slabs - 1)
    def _():
        for p in around:
            greet(s + 1, p)

    def send(src, dst, slot_from, slot_to, slab, patch):
        return pltpu.make_async_remote_copy(
            src_ref=src, dst_ref=dst, send_sem=send_sem.at[slot_from], recv_sem=recv_sem.at[slot_to],
            device_id=(slab, patch), device_id_type=MESH,
        )

    tail_c = send(tail_s, tail_r, 0, 0, s, right)
    head_c = send(head_s, head_r, 1, 1, s, left)
    zt_c = send(zt_s, zt_r, 2, 2, s, right)
    zh_c = send(zh_s, zh_r, 3, 3, s, left)
    down_c = [send(d_s, d_r.at[j], 4 + j, 4 + j, s + 1, p) for j, p in ((0, q), (2, left), (1, right))]
    up_c = [send(u_s, u_r.at[j], 7 + j, 7 + j, s - 1, p) for j, p in ((0, q), (2, left), (1, right))]

    count = margin_ref[0, 0]
    row = lax.broadcasted_iota(jnp.int32, (KMAX, KMAX), 0)
    col = lax.broadcasted_iota(jnp.int32, (KMAX, KMAX), 1)
    hit = (row == KMAX - count + col) & (col < count)
    place[...] = jnp.where(hit, 1.0, 0.0).astype(BF)

    first = solve(r_ref[0, 0].astype(BF), fac, m)
    tail_s[...] = nn(first[-1].astype(BF), place[...]).astype(BF)
    head_s[...] = first[0].astype(BF)

    pl.semaphore_wait(barrier, 2 + 3 * (s > 0).astype(jnp.int32) + 3 * (s < slabs - 1).astype(jnp.int32))
    tail_c.start()
    head_c.start()

    low = fac[:, :face]
    high = fac[m - face :, m - face :]
    k_tail = jnp.concatenate(
        [tn(low[m - KMAX :], fac[m - KMAX :, m - KMAX :]), tn(high, fac[m - face :, m - KMAX :])], axis=0
    )
    k_head = jnp.concatenate([tn(low, fac[:, :KMAX]), tn(high, fac[m - face :, :KMAX])], axis=0)
    zt_s[...] = nn(k_tail.astype(BF), place[...]).astype(BF)
    zh_s[...] = k_head.astype(BF)
    zt_c.start()
    zh_c.start()

    maps = jnp.concatenate([f_ref[0, 0], b_ref[0, 0]], axis=0)
    for k, part in enumerate(solve(maps, fac, m)):
        gt[:, k * KMAX : (k + 1) * KMAX] = part.astype(BF)

    tail_c.wait_recv()
    head_c.wait_recv()
    adj[...] = r_ref[0, 0]
    adj[:, :KMAX] = adj[:, :KMAX] - 0.5 * tail_r[...].astype(F32)
    adj[:, m - KMAX :] = adj[:, m - KMAX :] - 0.5 * nt(head_r[...], place[...])
    acc[...] = nt(adj[...].astype(BF), gt[...])

    def send_down():
        d_s[...] = acc[:, :face].astype(BF)
        for c in down_c:
            c.start()

    def send_up():
        u_s[...] = acc[:, face:].astype(BF)
        for c in up_c:
            c.start()

    @pl.when(s == 0)
    def _():
        send_down()

    zt_c.wait_recv()
    zh_c.wait_recv()
    zr[...] = nt(zh_r[...], place[...]).astype(BF)
    op_l = (0.5 * nt(gt[:, :KMAX], zt_r[...])).astype(BF)
    op_r = (0.5 * nt(gt[:, m - KMAX :], zr[...])).astype(BF)
    opd[:, :face] = -gt[:, :face]
    opd[:, face : 2 * face] = op_l[:, :face]
    opd[:, 2 * face :] = op_r[:, :face]
    opu[:, :face] = -gt[face:, m - face :]
    opu[:, face : 2 * face] = op_l[face:, face:]
    opu[:, 2 * face :] = op_r[face:, face:]

    def beside(ref):
        return jnp.concatenate([ref[0], ref[1], ref[2]], axis=1)

    @pl.when(s > 0)
    def _():
        for c in down_c:
            c.wait_recv()
        acc[...] += nt(beside(d_r), opd[...])

        @pl.when(s < slabs - 1)
        def _():
            send_down()

        @pl.when(s == slabs - 1)
        def _():
            send_up()

        adj[:, :face] = adj[:, :face] - d_r[0].astype(F32)
        adj[:, :KMAX] = adj[:, :KMAX] + 0.5 * nn(d_r[1], zt_r[:face])
        adj[:, m - KMAX :] = adj[:, m - KMAX :] + 0.5 * nn(d_r[2], zr[:face])

    @pl.when(s < slabs - 1)
    def _():
        for c in up_c:
            c.wait_recv()

        @pl.when(s > 0)
        def _():
            acc[:, face:] = acc[:, face:] + nt(beside(u_r), opu[...])
            send_up()

        adj[:, m - face :] = adj[:, m - face :] - u_r[0].astype(F32)
        adj[:, :KMAX] = adj[:, :KMAX] + 0.5 * nn(u_r[1], zt_r[face:])
        adj[:, m - KMAX :] = adj[:, m - KMAX :] + 0.5 * nn(u_r[2], zr[face:])

    for k, part in enumerate(solve(adj[...].astype(BF), fac, m)):
        out_ref[0, 0, :, k * KMAX : (k + 1) * KMAX] = part

    for c in (tail_c, head_c, zt_c, zh_c):
        c.wait_send()

    @pl.when(s < slabs - 1)
    def _():
        for c in down_c:
            c.wait_send()

    @pl.when(s > 0)
    def _():
        for c in up_c:
            c.wait_send()


def on_device(slabs, patches, right_side, inverse_factor, forward_trace, backward_trace, margin):
    cols, m = right_side.shape[2:]
    face = forward_trace.shape[2]
    wide = pltpu.VMEM((cols, KMAX), BF)
    square = pltpu.VMEM((2 * face, KMAX), BF)
    thin = pltpu.VMEM((cols, face), BF)
    three = pltpu.VMEM((3, cols, face), BF)
    vm = pl.BlockSpec(memory_space=pltpu.VMEM)
    return pl.pallas_call(
        functools.partial(kernel, slabs, patches),
        out_shape=jax.ShapeDtypeStruct(right_side.shape, F32),
        in_specs=[vm, vm, vm, vm, pl.BlockSpec(memory_space=pltpu.SMEM)],
        out_specs=vm,
        scratch_shapes=[
            wide, wide, square, square, thin, thin,
            wide, wide, square, square, three, three,
            pltpu.VMEM((cols, m), F32),
            pltpu.VMEM((cols, 2 * face), F32),
            pltpu.VMEM((2 * face, m), BF),
            pltpu.VMEM((2 * face, 3 * face), BF),
            pltpu.VMEM((face, 3 * face), BF),
            pltpu.VMEM((KMAX, KMAX), BF),
            square,
            pltpu.SemaphoreType.DMA((10,)),
            pltpu.SemaphoreType.DMA((10,)),
        ],
        compiler_params=pltpu.CompilerParams(collective_id=0, has_side_effects=True),
        name="sweeps",
    )(right_side, inverse_factor, forward_trace, backward_trace, margin)


def solution(mesh):
    four = P("slab", "patch", None, None)
    return jax.shard_map(
        functools.partial(on_device, mesh.shape["slab"], mesh.shape["patch"]),
        mesh=mesh,
        in_specs=(four, four, four, four, P("slab", "patch")),
        out_specs=four,
        check_vma=False,
    )
```

```python
import functools

import jax
import jax.numpy as jnp
from jax import lax
from jax.experimental import pallas as pl
from jax.experimental.pallas import tpu as pltpu
from jax.sharding import PartitionSpec as P

KMAX = 256
BF = jnp.bfloat16
F32 = jnp.float32
MESH = pl.DeviceIdType.MESH


def nt(a, b):
    return lax.dot_general(a, b, (((1,), (1,)), ((), ())), preferred_element_type=F32)


def nn(a, b):
    return lax.dot_general(a, b, (((1,), (0,)), ((), ())), preferred_element_type=F32)


def tn(a, b):
    return lax.dot_general(a, b, (((0,), (0,)), ((), ())), preferred_element_type=F32)


def solve(x, fac, m):
    half = jnp.concatenate(
        [nt(x[:, : i + KMAX], fac[i : i + KMAX, : i + KMAX]).astype(BF) for i in range(0, m, KMAX)],
        axis=1,
    )
    return [nn(half[:, k:], fac[k:, k : k + KMAX]) for k in range(0, m, KMAX)]


def kernel(
    slabs, patches, parts,
    r_hbm, l_hbm, f_hbm, b_hbm, margin_ref, out_ref,
    r_v, fac, maps,
    tail_s, head_s, zt_s, zh_s, d_s, u_s,
    tail_r, head_r, zt_r, zh_r, d_r, u_r,
    adj, acc, gt, opd, opu, place, zr,
    load_sem, send_sem, recv_sem, go_sem,
):
    s = lax.axis_index("slab")
    q = lax.axis_index("patch")
    left = lax.rem(q + patches - 1, patches)
    right = lax.rem(q + 1, patches)
    around = (left, right, q)
    m = fac.shape[-1]
    face = f_hbm.shape[-2]
    cols = r_v.shape[0]
    step = cols // parts
    first_slab, last_slab = s == 0, s == slabs - 1
    inner_low, inner_high = s > 0, s < slabs - 1

    loads = [
        pltpu.make_async_copy(r_hbm.at[0, 0], r_v, load_sem.at[0]),
        pltpu.make_async_copy(l_hbm.at[0, 0], fac, load_sem.at[1]),
        pltpu.make_async_copy(f_hbm.at[0, 0], maps.at[:face], load_sem.at[2]),
        pltpu.make_async_copy(b_hbm.at[0, 0], maps.at[face:], load_sem.at[3]),
    ]
    for c in loads:
        c.start()

    barrier = pltpu.get_barrier_semaphore()

    def greet(slab, patch):
        pl.semaphore_signal(barrier, inc=1, device_id=(slab, patch), device_id_type=MESH)

    greet(s, left)
    greet(s, right)

    @pl.when(inner_low)
    def _():
        for p in around:
            greet(s - 1, p)

    @pl.when(inner_high)
    def _():
        for p in around:
            greet(s + 1, p)

    slot = [0]

    def send(src, dst, slab, patch):
        n = slot[0]
        slot[0] += 1
        return pltpu.make_async_remote_copy(
            src_ref=src, dst_ref=dst, send_sem=send_sem.at[n], recv_sem=recv_sem.at[n],
            device_id=(slab, patch), device_id_type=MESH,
        )

    rows = [pl.ds(c * step, step) for c in range(parts)]
    tail_c = [send(tail_s.at[w], tail_r.at[w], s, right) for w in rows]
    head_c = [send(head_s.at[w], head_r.at[w], s, left) for w in rows]
    low_rows, high_rows = pl.ds(0, face), pl.ds(face, face)
    zd_c = [send(zt_s.at[low_rows], zt_r.at[low_rows], s, right), send(zh_s.at[low_rows], zh_r.at[low_rows], s, left)]
    zu_c = [send(zt_s.at[high_rows], zt_r.at[high_rows], s, right), send(zh_s.at[high_rows], zh_r.at[high_rows], s, left)]
    targets = ((2, left), (1, right), (0, q))
    down_c = [[send(d_s.at[w], d_r.at[j, w], s + 1, p) for j, p in targets] for w in rows]
    up_c = [[send(u_s.at[w], u_r.at[j, w], s - 1, p) for j, p in targets] for w in rows]

    count = margin_ref[0, 0]
    row = lax.broadcasted_iota(jnp.int32, (KMAX, KMAX), 0)
    col = lax.broadcasted_iota(jnp.int32, (KMAX, KMAX), 1)
    hit = (row == KMAX - count + col) & (col < count)
    place[...] = jnp.where(hit, 1.0, 0.0).astype(BF)

    loads[0].wait()
    loads[1].wait()
    first = solve(r_v[...].astype(BF), fac, m)
    tail_s[...] = nn(first[-1].astype(BF), place[...]).astype(BF)
    head_s[...] = first[0].astype(BF)

    pl.semaphore_wait(barrier, 2 + 3 * inner_low.astype(jnp.int32) + 3 * inner_high.astype(jnp.int32))

    def send_first():
        for a, b in zip(tail_c, head_c):
            a.start()
            b.start()

    @pl.when(s != 1)
    def _():
        send_first()

    loads[2].wait()
    loads[3].wait()
    for k, part in enumerate(solve(maps[...], fac, m)):
        gt[:, k * KMAX : (k + 1) * KMAX] = part.astype(BF)

    low = fac[:, :face]
    high = fac[m - face :, m - face :]
    k_tail = jnp.concatenate(
        [tn(low[m - KMAX :], fac[m - KMAX :, m - KMAX :]), tn(high, fac[m - face :, m - KMAX :])], axis=0
    )
    k_head = jnp.concatenate([tn(low, fac[:, :KMAX]), tn(high, fac[m - face :, :KMAX])], axis=0)
    zt_s[...] = nn(k_tail.astype(BF), place[...]).astype(BF)
    zh_s[...] = k_head.astype(BF)

    @pl.when(s == 1)
    def _():
        pl.semaphore_wait(go_sem, 1)
        send_first()

    @pl.when(inner_low)
    def _():
        for c in zd_c:
            c.start()

    @pl.when(inner_low & inner_high)
    def _():
        for c in zu_c:
            c.start()

    def send_down(c):
        w = rows[c]
        d_s[w] = acc[w, :face].astype(BF)
        for x in down_c[c]:
            x.start()

    def send_up(c):
        w = rows[c]
        u_s[w] = acc[w, face:].astype(BF)
        for x in up_c[c]:
            x.start()

    for c, w in enumerate(rows):
        tail_c[c].wait_recv()
        head_c[c].wait_recv()
        adj[w, :] = r_v[w, :]
        adj[w, :KMAX] = adj[w, :KMAX] - 0.5 * tail_r[w].astype(F32)
        adj[w, m - KMAX :] = adj[w, m - KMAX :] - 0.5 * nt(head_r[w], place[...])
        acc[w, :face] = nt(adj[w, :].astype(BF), gt[:face])

        @pl.when(first_slab)
        def _():
            send_down(c)
            tail_c[c].wait_send()
            head_c[c].wait_send()
            if c == 0:
                pl.semaphore_signal(go_sem, inc=1, device_id=(s + 1, q), device_id_type=MESH)

    @pl.when(first_slab)
    def _():
        for c in zu_c:
            c.start()

    acc[:, face:] = nt(adj[...].astype(BF), gt[face:])

    @pl.when(inner_low)
    def _():
        for c in zd_c:
            c.wait_recv()
        zr[low_rows] = nt(zh_r[low_rows], place[...]).astype(BF)
        opd[:face, :] = (-gt[:, :face].astype(F32)).T.astype(BF)
        opd[face : 2 * face, :] = (0.5 * nt(zt_r[low_rows], gt[:, :KMAX])).astype(BF)
        opd[2 * face :, :] = (0.5 * nt(zr[low_rows], gt[:, m - KMAX :])).astype(BF)

    def make_up():
        for c in zu_c:
            c.wait_recv()
        zr[high_rows] = nt(zh_r[high_rows], place[...]).astype(BF)

        @pl.when(inner_low)
        def _():
            opu[:face, :] = (-gt[face:, m - face :].astype(F32)).T.astype(BF)
            opu[face : 2 * face, :] = (0.5 * nt(zt_r[high_rows], gt[face:, :KMAX])).astype(BF)
            opu[2 * face :, :] = (0.5 * nt(zr[high_rows], gt[face:, m - KMAX :])).astype(BF)

    def beside(ref, w):
        return jnp.concatenate([ref[0, w], ref[1, w], ref[2, w]], axis=1)

    @pl.when(inner_low)
    def _():
        for c, w in enumerate(rows):
            for x in down_c[c]:
                x.wait_recv()

            @pl.when(inner_high)
            def _():
                acc[w, :face] += nn(beside(d_r, w), opd[:, :face])
                send_down(c)

            @pl.when(last_slab)
            def _():
                acc[w, face:] += nn(beside(d_r, w), opd[:, face:])
                send_up(c)

        @pl.when(inner_high)
        def _():
            every = pl.ds(0, cols)
            acc[:, face:] += nn(beside(d_r, every), opd[:, face:])

        adj[:, :face] = adj[:, :face] - d_r[0].astype(F32)
        adj[:, :KMAX] = adj[:, :KMAX] + 0.5 * nn(d_r[1], zt_r[low_rows])
        adj[:, m - KMAX :] = adj[:, m - KMAX :] + 0.5 * nn(d_r[2], zr[low_rows])

    @pl.when(inner_high)
    def _():
        make_up()
        for c, w in enumerate(rows):
            for x in up_c[c]:
                x.wait_recv()

            @pl.when(inner_low)
            def _():
                acc[w, face:] += nn(beside(u_r, w), opu[...])
                send_up(c)

        adj[:, m - face :] = adj[:, m - face :] - u_r[0].astype(F32)
        adj[:, :KMAX] = adj[:, :KMAX] + 0.5 * nn(u_r[1], zt_r[high_rows])
        adj[:, m - KMAX :] = adj[:, m - KMAX :] + 0.5 * nn(u_r[2], zr[high_rows])

    for k, part in enumerate(solve(adj[...].astype(BF), fac, m)):
        out_ref[0, 0, :, k * KMAX : (k + 1) * KMAX] = part

    @pl.when(inner_low)
    def _():
        for c in tail_c + head_c + zd_c:
            c.wait_send()
        for group in up_c:
            for x in group:
                x.wait_send()

    @pl.when(inner_high)
    def _():
        for c in zu_c:
            c.wait_send()
        for group in down_c:
            for x in group:
                x.wait_send()


def on_device(slabs, patches, right_side, inverse_factor, forward_trace, backward_trace, margin):
    cols, m = right_side.shape[2:]
    face = forward_trace.shape[2]
    parts = 2
    copies = 2 * parts + 4 + 6 * parts
    wide = pltpu.VMEM((cols, KMAX), BF)
    square = pltpu.VMEM((2 * face, KMAX), BF)
    thin = pltpu.VMEM((cols, face), BF)
    three = pltpu.VMEM((3, cols, face), BF)
    hbm = pl.BlockSpec(memory_space=pltpu.HBM)
    return pl.pallas_call(
        functools.partial(kernel, slabs, patches, parts),
        out_shape=jax.ShapeDtypeStruct(right_side.shape, F32),
        in_specs=[hbm, hbm, hbm, hbm, pl.BlockSpec(memory_space=pltpu.SMEM)],
        out_specs=pl.BlockSpec(memory_space=pltpu.VMEM),
        scratch_shapes=[
            pltpu.VMEM((cols, m), F32),
            pltpu.VMEM((m, m), BF),
            pltpu.VMEM((2 * face, m), BF),
            wide, wide, square, square, thin, thin,
            wide, wide, square, square, three, three,
            pltpu.VMEM((cols, m), F32),
            pltpu.VMEM((cols, 2 * face), F32),
            pltpu.VMEM((2 * face, m), BF),
            pltpu.VMEM((3 * face, 2 * face), BF),
            pltpu.VMEM((3 * face, face), BF),
            pltpu.VMEM((KMAX, KMAX), BF),
            square,
            pltpu.SemaphoreType.DMA((4,)),
            pltpu.SemaphoreType.DMA((copies,)),
            pltpu.SemaphoreType.DMA((copies,)),
            pltpu.SemaphoreType.REGULAR,
        ],
        compiler_params=pltpu.CompilerParams(collective_id=0, has_side_effects=True),
        name="sweeps",
    )(right_side, inverse_factor, forward_trace, backward_trace, margin)


def solution(mesh):
    four = P("slab", "patch", None, None)
    return jax.shard_map(
        functools.partial(on_device, mesh.shape["slab"], mesh.shape["patch"]),
        mesh=mesh,
        in_specs=(four, four, four, four, P("slab", "patch")),
        out_specs=four,
        check_vma=False,
    )
```

```python
import functools

import jax
import jax.numpy as jnp
from jax import lax
from jax.experimental import pallas as pl
from jax.experimental.pallas import tpu as pltpu
from jax.sharding import PartitionSpec as P

KMAX = 256
BF = jnp.bfloat16
F32 = jnp.float32
MESH = pl.DeviceIdType.MESH


def nt(a, b):
    return lax.dot_general(a, b, (((1,), (1,)), ((), ())), preferred_element_type=F32)


def nn(a, b):
    return lax.dot_general(a, b, (((1,), (0,)), ((), ())), preferred_element_type=F32)


def tn(a, b):
    return lax.dot_general(a, b, (((0,), (0,)), ((), ())), preferred_element_type=F32)


def solve(x, fac, m):
    half = jnp.concatenate(
        [nt(x[:, : i + KMAX], fac[i : i + KMAX, : i + KMAX]).astype(BF) for i in range(0, m, KMAX)],
        axis=1,
    )
    return [nn(half[:, k:], fac[k:, k : k + KMAX]) for k in range(0, m, KMAX)]


def kernel(
    slabs, patches, parts,
    r_hbm, l_hbm, f_hbm, b_hbm, margin_ref, out_ref,
    r_v, fac, maps,
    tail_s, head_s, zt_s, zh_s, d_s, u_s,
    tail_r, head_r, zt_r, zh_r, d_r, u_r,
    adj, acc, gt, opd, opu, place, zr,
    load_sem, send_sem, recv_sem,
):
    s = lax.axis_index("slab")
    q = lax.axis_index("patch")
    left = lax.rem(q + patches - 1, patches)
    right = lax.rem(q + 1, patches)
    around = (left, right, q)
    m = fac.shape[-1]
    face = f_hbm.shape[-2]
    cols = r_v.shape[0]
    step = cols // parts
    first_slab, last_slab = s == 0, s == slabs - 1
    inner_low, inner_high = s > 0, s < slabs - 1

    loads = [
        pltpu.make_async_copy(r_hbm.at[0, 0], r_v, load_sem.at[0]),
        pltpu.make_async_copy(l_hbm.at[0, 0], fac, load_sem.at[1]),
        pltpu.make_async_copy(f_hbm.at[0, 0], maps.at[:face], load_sem.at[2]),
        pltpu.make_async_copy(b_hbm.at[0, 0], maps.at[face:], load_sem.at[3]),
    ]
    for c in loads:
        c.start()

    barrier = pltpu.get_barrier_semaphore()

    def greet(slab, patch):
        pl.semaphore_signal(barrier, inc=1, device_id=(slab, patch), device_id_type=MESH)

    greet(s, left)
    greet(s, right)

    @pl.when(inner_low)
    def _():
        for p in around:
            greet(s - 1, p)

    @pl.when(inner_high)
    def _():
        for p in around:
            greet(s + 1, p)

    slot = [0]

    def send(src, dst, slab, patch):
        n = slot[0]
        slot[0] += 1
        return pltpu.make_async_remote_copy(
            src_ref=src, dst_ref=dst, send_sem=send_sem.at[n], recv_sem=recv_sem.at[n],
            device_id=(slab, patch), device_id_type=MESH,
        )

    rows = [pl.ds(c * step, step) for c in range(parts)]
    tail_c = [send(tail_s.at[w], tail_r.at[w], s, right) for w in rows]
    head_c = [send(head_s.at[w], head_r.at[w], s, left) for w in rows]
    low_rows, high_rows = pl.ds(0, face), pl.ds(face, face)
    zd_c = [send(zt_s.at[low_rows], zt_r.at[low_rows], s, right), send(zh_s.at[low_rows], zh_r.at[low_rows], s, left)]
    zu_c = [send(zt_s.at[high_rows], zt_r.at[high_rows], s, right), send(zh_s.at[high_rows], zh_r.at[high_rows], s, left)]
    targets = ((2, left), (1, right), (0, q))
    down_c = [[send(d_s.at[w], d_r.at[j, w], s + 1, p) for j, p in targets] for w in rows]
    up_c = [[send(u_s.at[w], u_r.at[j, w], s - 1, p) for j, p in targets] for w in rows]

    count = margin_ref[0, 0]
    row = lax.broadcasted_iota(jnp.int32, (KMAX, KMAX), 0)
    col = lax.broadcasted_iota(jnp.int32, (KMAX, KMAX), 1)
    hit = (row == KMAX - count + col) & (col < count)
    place[...] = jnp.where(hit, 1.0, 0.0).astype(BF)

    loads[0].wait()
    loads[1].wait()
    first = solve(r_v[...].astype(BF), fac, m)
    tail_s[...] = nn(first[-1].astype(BF), place[...]).astype(BF)
    head_s[...] = first[0].astype(BF)

    pl.semaphore_wait(barrier, 2 + 3 * inner_low.astype(jnp.int32) + 3 * inner_high.astype(jnp.int32))

    for a, b in zip(tail_c, head_c):
        a.start()
        b.start()

    loads[2].wait()
    loads[3].wait()
    for k, part in enumerate(solve(maps[...], fac, m)):
        gt[:, k * KMAX : (k + 1) * KMAX] = part.astype(BF)

    low = fac[:, :face]
    high = fac[m - face :, m - face :]
    k_tail = jnp.concatenate(
        [tn(low[m - KMAX :], fac[m - KMAX :, m - KMAX :]), tn(high, fac[m - face :, m - KMAX :])], axis=0
    )
    k_head = jnp.concatenate([tn(low, fac[:, :KMAX]), tn(high, fac[m - face :, :KMAX])], axis=0)
    zt_s[...] = nn(k_tail.astype(BF), place[...]).astype(BF)
    zh_s[...] = k_head.astype(BF)

    @pl.when(inner_low)
    def _():
        for c in zd_c:
            c.start()

    @pl.when(inner_low & inner_high)
    def _():
        for c in zu_c:
            c.start()

    def send_down(c):
        w = rows[c]
        d_s[w] = acc[w, :face].astype(BF)
        for x in down_c[c]:
            x.start()

    def send_up(c):
        w = rows[c]
        u_s[w] = acc[w, face:].astype(BF)
        for x in up_c[c]:
            x.start()

    for c, w in enumerate(rows):
        tail_c[c].wait_recv()
        head_c[c].wait_recv()
        adj[w, :] = r_v[w, :]
        adj[w, :KMAX] = adj[w, :KMAX] - 0.5 * tail_r[w].astype(F32)
        adj[w, m - KMAX :] = adj[w, m - KMAX :] - 0.5 * nt(head_r[w], place[...])
        acc[w, :face] = nt(adj[w, :].astype(BF), gt[:face])

        @pl.when(first_slab)
        def _():
            send_down(c)

    @pl.when(first_slab)
    def _():
        for c in zu_c:
            c.start()

    acc[:, face:] = nt(adj[...].astype(BF), gt[face:])

    @pl.when(inner_low)
    def _():
        for c in zd_c:
            c.wait_recv()
        zr[low_rows] = nt(zh_r[low_rows], place[...]).astype(BF)
        opd[:face, :] = (-gt[:, :face].astype(F32)).T.astype(BF)
        opd[face : 2 * face, :] = (0.5 * nt(zt_r[low_rows], gt[:, :KMAX])).astype(BF)
        opd[2 * face :, :] = (0.5 * nt(zr[low_rows], gt[:, m - KMAX :])).astype(BF)

    def make_up():
        for c in zu_c:
            c.wait_recv()
        zr[high_rows] = nt(zh_r[high_rows], place[...]).astype(BF)

        @pl.when(inner_low)
        def _():
            opu[:face, :] = (-gt[face:, m - face :].astype(F32)).T.astype(BF)
            opu[face : 2 * face, :] = (0.5 * nt(zt_r[high_rows], gt[face:, :KMAX])).astype(BF)
            opu[2 * face :, :] = (0.5 * nt(zr[high_rows], gt[face:, m - KMAX :])).astype(BF)

    def beside(ref, w):
        return jnp.concatenate([ref[0, w], ref[1, w], ref[2, w]], axis=1)

    @pl.when(inner_low)
    def _():
        for c, w in enumerate(rows):
            for x in down_c[c]:
                x.wait_recv()

            @pl.when(inner_high)
            def _():
                acc[w, :face] += nn(beside(d_r, w), opd[:, :face])
                send_down(c)

            @pl.when(last_slab)
            def _():
                acc[w, face:] += nn(beside(d_r, w), opd[:, face:])
                send_up(c)

        @pl.when(inner_high)
        def _():
            every = pl.ds(0, cols)
            acc[:, face:] += nn(beside(d_r, every), opd[:, face:])

        adj[:, :face] = adj[:, :face] - d_r[0].astype(F32)
        adj[:, :KMAX] = adj[:, :KMAX] + 0.5 * nn(d_r[1], zt_r[low_rows])
        adj[:, m - KMAX :] = adj[:, m - KMAX :] + 0.5 * nn(d_r[2], zr[low_rows])

    @pl.when(inner_high)
    def _():
        make_up()
        for c, w in enumerate(rows):
            for x in up_c[c]:
                x.wait_recv()

            @pl.when(inner_low)
            def _():
                acc[w, face:] += nn(beside(u_r, w), opu[...])
                send_up(c)

        adj[:, m - face :] = adj[:, m - face :] - u_r[0].astype(F32)
        adj[:, :KMAX] = adj[:, :KMAX] + 0.5 * nn(u_r[1], zt_r[high_rows])
        adj[:, m - KMAX :] = adj[:, m - KMAX :] + 0.5 * nn(u_r[2], zr[high_rows])

    for k, part in enumerate(solve(adj[...].astype(BF), fac, m)):
        out_ref[0, 0, :, k * KMAX : (k + 1) * KMAX] = part

    for c in tail_c + head_c:
        c.wait_send()

    @pl.when(inner_low)
    def _():
        for c in zd_c:
            c.wait_send()
        for group in up_c:
            for x in group:
                x.wait_send()

    @pl.when(inner_high)
    def _():
        for c in zu_c:
            c.wait_send()
        for group in down_c:
            for x in group:
                x.wait_send()


def on_device(slabs, patches, right_side, inverse_factor, forward_trace, backward_trace, margin):
    cols, m = right_side.shape[2:]
    face = forward_trace.shape[2]
    parts = 4
    copies = 2 * parts + 4 + 6 * parts
    wide = pltpu.VMEM((cols, KMAX), BF)
    square = pltpu.VMEM((2 * face, KMAX), BF)
    thin = pltpu.VMEM((cols, face), BF)
    three = pltpu.VMEM((3, cols, face), BF)
    hbm = pl.BlockSpec(memory_space=pltpu.HBM)
    return pl.pallas_call(
        functools.partial(kernel, slabs, patches, parts),
        out_shape=jax.ShapeDtypeStruct(right_side.shape, F32),
        in_specs=[hbm, hbm, hbm, hbm, pl.BlockSpec(memory_space=pltpu.SMEM)],
        out_specs=pl.BlockSpec(memory_space=pltpu.VMEM),
        scratch_shapes=[
            pltpu.VMEM((cols, m), F32),
            pltpu.VMEM((m, m), BF),
            pltpu.VMEM((2 * face, m), BF),
            wide, wide, square, square, thin, thin,
            wide, wide, square, square, three, three,
            pltpu.VMEM((cols, m), F32),
            pltpu.VMEM((cols, 2 * face), F32),
            pltpu.VMEM((2 * face, m), BF),
            pltpu.VMEM((3 * face, 2 * face), BF),
            pltpu.VMEM((3 * face, face), BF),
            pltpu.VMEM((KMAX, KMAX), BF),
            square,
            pltpu.SemaphoreType.DMA((4,)),
            pltpu.SemaphoreType.DMA((copies,)),
            pltpu.SemaphoreType.DMA((copies,)),
        ],
        compiler_params=pltpu.CompilerParams(collective_id=0, has_side_effects=True),
        name="sweeps",
    )(right_side, inverse_factor, forward_trace, backward_trace, margin)


def solution(mesh):
    four = P("slab", "patch", None, None)
    return jax.shard_map(
        functools.partial(on_device, mesh.shape["slab"], mesh.shape["patch"]),
        mesh=mesh,
        in_specs=(four, four, four, four, P("slab", "patch")),
        out_specs=four,
        check_vma=False,
    )
```

```python
import functools

import jax
import jax.numpy as jnp
from jax import lax
from jax.experimental import pallas as pl
from jax.experimental.pallas import tpu as pltpu
from jax.sharding import PartitionSpec as P

KMAX = 256
BF = jnp.bfloat16
F32 = jnp.float32
MESH = pl.DeviceIdType.MESH


def nt(a, b):
    return lax.dot_general(a, b, (((1,), (1,)), ((), ())), preferred_element_type=F32)


def nn(a, b):
    return lax.dot_general(a, b, (((1,), (0,)), ((), ())), preferred_element_type=F32)


def tn(a, b):
    return lax.dot_general(a, b, (((0,), (0,)), ((), ())), preferred_element_type=F32)


def halfway(x, fac, m):
    return jnp.concatenate(
        [nt(x[:, : i + KMAX], fac[i : i + KMAX, : i + KMAX]).astype(BF) for i in range(0, m, KMAX)],
        axis=1,
    )


def solve(x, fac, m):
    half = halfway(x, fac, m)
    return [nn(half[:, k:], fac[k:, k : k + KMAX]) for k in range(0, m, KMAX)]


def finish(half_ref, l_ref, out_ref, held, sem):
    m = half_ref.shape[1]
    copies = []
    for n, k in enumerate(range(0, m, KMAX)):
        held[n] = nn(half_ref[:, k:], l_ref[0, 0, k:, k : k + KMAX])
        copies.append(pltpu.make_async_copy(held.at[n], out_ref.at[0, 0, :, k : k + KMAX], sem.at[n]))
        copies[-1].start()
    for c in copies:
        c.wait()


def kernel(
    slabs, patches, parts,
    r_hbm, l_hbm, f_hbm, b_hbm, margin_ref, out_ref,
    r_v, fac, maps,
    tail_s, head_s, zt_s, zh_s, d_s, u_s,
    tail_r, head_r, zt_r, zh_r, d_r, u_r,
    adj, acc, gt, opd, opu, place, zr,
    load_sem, send_sem, recv_sem,
):
    s = lax.axis_index("slab")
    q = lax.axis_index("patch")
    left = lax.rem(q + patches - 1, patches)
    right = lax.rem(q + 1, patches)
    around = (left, right, q)
    m = fac.shape[-1]
    face = f_hbm.shape[-2]
    cols = r_v.shape[0]
    step = cols // parts
    first_slab, last_slab = s == 0, s == slabs - 1
    inner_low, inner_high = s > 0, s < slabs - 1

    loads = [
        pltpu.make_async_copy(r_hbm.at[0, 0], r_v, load_sem.at[0]),
        pltpu.make_async_copy(l_hbm.at[0, 0], fac, load_sem.at[1]),
        pltpu.make_async_copy(f_hbm.at[0, 0], maps.at[:face], load_sem.at[2]),
        pltpu.make_async_copy(b_hbm.at[0, 0], maps.at[face:], load_sem.at[3]),
    ]
    for c in loads:
        c.start()

    barrier = pltpu.get_barrier_semaphore()

    def greet(slab, patch):
        pl.semaphore_signal(barrier, inc=1, device_id=(slab, patch), device_id_type=MESH)

    greet(s, left)
    greet(s, right)

    @pl.when(inner_low)
    def _():
        for p in around:
            greet(s - 1, p)

    @pl.when(inner_high)
    def _():
        for p in around:
            greet(s + 1, p)

    slot = [0]

    def send(src, dst, slab, patch):
        n = slot[0]
        slot[0] += 1
        return pltpu.make_async_remote_copy(
            src_ref=src, dst_ref=dst, send_sem=send_sem.at[n], recv_sem=recv_sem.at[n],
            device_id=(slab, patch), device_id_type=MESH,
        )

    rows = [pl.ds(c * step, step) for c in range(parts)]
    tail_c = [send(tail_s.at[w], tail_r.at[w], s, right) for w in rows]
    head_c = [send(head_s.at[w], head_r.at[w], s, left) for w in rows]
    low_rows, high_rows = pl.ds(0, face), pl.ds(face, face)
    zd_c = [send(zt_s.at[low_rows], zt_r.at[low_rows], s, right), send(zh_s.at[low_rows], zh_r.at[low_rows], s, left)]
    zu_c = [send(zt_s.at[high_rows], zt_r.at[high_rows], s, right), send(zh_s.at[high_rows], zh_r.at[high_rows], s, left)]
    targets = ((2, left), (1, right), (0, q))
    down_c = [[send(d_s.at[w], d_r.at[j, w], s + 1, p) for j, p in targets] for w in rows]
    up_c = [[send(u_s.at[w], u_r.at[j, w], s - 1, p) for j, p in targets] for w in rows]

    count = margin_ref[0, 0]
    row = lax.broadcasted_iota(jnp.int32, (KMAX, KMAX), 0)
    col = lax.broadcasted_iota(jnp.int32, (KMAX, KMAX), 1)
    hit = (row == KMAX - count + col) & (col < count)
    place[...] = jnp.where(hit, 1.0, 0.0).astype(BF)

    loads[0].wait()
    loads[1].wait()
    first = solve(r_v[...].astype(BF), fac, m)
    tail_s[...] = nn(first[-1].astype(BF), place[...]).astype(BF)
    head_s[...] = first[0].astype(BF)

    pl.semaphore_wait(barrier, 2 + 3 * inner_low.astype(jnp.int32) + 3 * inner_high.astype(jnp.int32))

    for a, b in zip(tail_c, head_c):
        a.start()
        b.start()

    loads[2].wait()
    loads[3].wait()
    for k, part in enumerate(solve(maps[...], fac, m)):
        gt[:, k * KMAX : (k + 1) * KMAX] = part.astype(BF)

    low = fac[:, :face]
    high = fac[m - face :, m - face :]
    k_tail = jnp.concatenate(
        [tn(low[m - KMAX :], fac[m - KMAX :, m - KMAX :]), tn(high, fac[m - face :, m - KMAX :])], axis=0
    )
    k_head = jnp.concatenate([tn(low, fac[:, :KMAX]), tn(high, fac[m - face :, :KMAX])], axis=0)
    zt_s[...] = nn(k_tail.astype(BF), place[...]).astype(BF)
    zh_s[...] = k_head.astype(BF)

    @pl.when(inner_low)
    def _():
        for c in zd_c:
            c.start()

    @pl.when(inner_low & inner_high)
    def _():
        for c in zu_c:
            c.start()

    def send_down(c):
        w = rows[c]
        d_s[w] = acc[w, :face].astype(BF)
        for x in down_c[c]:
            x.start()

    def send_up(c):
        w = rows[c]
        u_s[w] = acc[w, face:].astype(BF)
        for x in up_c[c]:
            x.start()

    for c, w in enumerate(rows):
        tail_c[c].wait_recv()
        head_c[c].wait_recv()
        adj[w, :] = r_v[w, :]
        adj[w, :KMAX] = adj[w, :KMAX] - 0.5 * tail_r[w].astype(F32)
        adj[w, m - KMAX :] = adj[w, m - KMAX :] - 0.5 * nt(head_r[w], place[...])
        acc[w, :face] = nt(adj[w, :].astype(BF), gt[:face])

        @pl.when(first_slab)
        def _():
            send_down(c)

    @pl.when(first_slab)
    def _():
        for c in zu_c:
            c.start()

    acc[:, face:] = nt(adj[...].astype(BF), gt[face:])

    @pl.when(inner_low)
    def _():
        for c in zd_c:
            c.wait_recv()
        zr[low_rows] = nt(zh_r[low_rows], place[...]).astype(BF)
        opd[:face, :] = (-gt[:, :face].astype(F32)).T.astype(BF)
        opd[face : 2 * face, :] = (0.5 * nt(zt_r[low_rows], gt[:, :KMAX])).astype(BF)
        opd[2 * face :, :] = (0.5 * nt(zr[low_rows], gt[:, m - KMAX :])).astype(BF)

    def make_up():
        for c in zu_c:
            c.wait_recv()
        zr[high_rows] = nt(zh_r[high_rows], place[...]).astype(BF)

        @pl.when(inner_low)
        def _():
            opu[:face, :] = (-gt[face:, m - face :].astype(F32)).T.astype(BF)
            opu[face : 2 * face, :] = (0.5 * nt(zt_r[high_rows], gt[face:, :KMAX])).astype(BF)
            opu[2 * face :, :] = (0.5 * nt(zr[high_rows], gt[face:, m - KMAX :])).astype(BF)

    def beside(ref, w):
        return jnp.concatenate([ref[0, w], ref[1, w], ref[2, w]], axis=1)

    @pl.when(inner_low)
    def _():
        for c, w in enumerate(rows):
            for x in down_c[c]:
                x.wait_recv()

            @pl.when(inner_high)
            def _():
                acc[w, :face] += nn(beside(d_r, w), opd[:, :face])
                send_down(c)

            @pl.when(last_slab)
            def _():
                acc[w, face:] += nn(beside(d_r, w), opd[:, face:])
                send_up(c)

        @pl.when(inner_high)
        def _():
            every = pl.ds(0, cols)
            acc[:, face:] += nn(beside(d_r, every), opd[:, face:])

        adj[:, :face] = adj[:, :face] - d_r[0].astype(F32)
        adj[:, :KMAX] = adj[:, :KMAX] + 0.5 * nn(d_r[1], zt_r[low_rows])
        adj[:, m - KMAX :] = adj[:, m - KMAX :] + 0.5 * nn(d_r[2], zr[low_rows])

    @pl.when(inner_high)
    def _():
        make_up()
        for c, w in enumerate(rows):
            for x in up_c[c]:
                x.wait_recv()

            @pl.when(inner_low)
            def _():
                acc[w, face:] += nn(beside(u_r, w), opu[...])
                send_up(c)

        adj[:, m - face :] = adj[:, m - face :] - u_r[0].astype(F32)
        adj[:, :KMAX] = adj[:, :KMAX] + 0.5 * nn(u_r[1], zt_r[high_rows])
        adj[:, m - KMAX :] = adj[:, m - KMAX :] + 0.5 * nn(u_r[2], zr[high_rows])

    out_ref[...] = halfway(adj[...].astype(BF), fac, m)

    for c in tail_c + head_c:
        c.wait_send()

    @pl.when(inner_low)
    def _():
        for c in zd_c:
            c.wait_send()
        for group in up_c:
            for x in group:
                x.wait_send()

    @pl.when(inner_high)
    def _():
        for c in zu_c:
            c.wait_send()
        for group in down_c:
            for x in group:
                x.wait_send()


def on_device(slabs, patches, right_side, inverse_factor, forward_trace, backward_trace, margin):
    cols, m = right_side.shape[2:]
    face = forward_trace.shape[2]
    parts = 4
    copies = 2 * parts + 4 + 6 * parts
    wide = pltpu.VMEM((cols, KMAX), BF)
    square = pltpu.VMEM((2 * face, KMAX), BF)
    thin = pltpu.VMEM((cols, face), BF)
    three = pltpu.VMEM((3, cols, face), BF)
    hbm = pl.BlockSpec(memory_space=pltpu.HBM)
    half = pl.pallas_call(
        functools.partial(kernel, slabs, patches, parts),
        out_shape=jax.ShapeDtypeStruct((cols, m), BF),
        in_specs=[hbm, hbm, hbm, hbm, pl.BlockSpec(memory_space=pltpu.SMEM)],
        out_specs=pl.BlockSpec(memory_space=pltpu.VMEM),
        scratch_shapes=[
            pltpu.VMEM((cols, m), F32),
            pltpu.VMEM((m, m), BF),
            pltpu.VMEM((2 * face, m), BF),
            wide, wide, square, square, thin, thin,
            wide, wide, square, square, three, three,
            pltpu.VMEM((cols, m), F32),
            pltpu.VMEM((cols, 2 * face), F32),
            pltpu.VMEM((2 * face, m), BF),
            pltpu.VMEM((3 * face, 2 * face), BF),
            pltpu.VMEM((3 * face, face), BF),
            pltpu.VMEM((KMAX, KMAX), BF),
            square,
            pltpu.SemaphoreType.DMA((4,)),
            pltpu.SemaphoreType.DMA((copies,)),
            pltpu.SemaphoreType.DMA((copies,)),
        ],
        compiler_params=pltpu.CompilerParams(collective_id=0, has_side_effects=True),
        name="sweeps",
    )(right_side, inverse_factor, forward_trace, backward_trace, margin)
    return pl.pallas_call(
        finish,
        out_shape=jax.ShapeDtypeStruct(right_side.shape, F32),
        in_specs=[pl.BlockSpec(memory_space=pltpu.VMEM)] * 2,
        out_specs=hbm,
        scratch_shapes=[pltpu.VMEM((m // KMAX, cols, KMAX), F32), pltpu.SemaphoreType.DMA((m // KMAX,))],
        compiler_params=pltpu.CompilerParams(vmem_limit_bytes=16 << 20),
        name="finish",
    )(half, inverse_factor)


def solution(mesh):
    four = P("slab", "patch", None, None)
    return jax.shard_map(
        functools.partial(on_device, mesh.shape["slab"], mesh.shape["patch"]),
        mesh=mesh,
        in_specs=(four, four, four, four, P("slab", "patch")),
        out_specs=four,
        check_vma=False,
    )
```

```python
import functools

import jax
import jax.numpy as jnp
from jax import lax
from jax.experimental import pallas as pl
from jax.experimental.pallas import tpu as pltpu
from jax.sharding import PartitionSpec as P

KMAX = 256
BF = jnp.bfloat16
F32 = jnp.float32
MESH = pl.DeviceIdType.MESH


def nt(a, b):
    return lax.dot_general(a, b, (((1,), (1,)), ((), ())), preferred_element_type=F32)


def nn(a, b):
    return lax.dot_general(a, b, (((1,), (0,)), ((), ())), preferred_element_type=F32)


def tn(a, b):
    return lax.dot_general(a, b, (((0,), (0,)), ((), ())), preferred_element_type=F32)


def halfway(x, fac, m):
    return jnp.concatenate(
        [nt(x[:, : i + KMAX], fac[i : i + KMAX, : i + KMAX]).astype(BF) for i in range(0, m, KMAX)],
        axis=1,
    )


def solve(x, fac, m):
    half = halfway(x, fac, m)
    return [nn(half[:, k:], fac[k:, k : k + KMAX]) for k in range(0, m, KMAX)]


def finish(half_ref, l_ref, out_ref, held, sem):
    m = half_ref.shape[1]
    copies = []
    for n, k in enumerate(range(0, m, KMAX)):
        held[n] = nn(half_ref[:, k:], l_ref[0, 0, k:, k : k + KMAX])
        copies.append(pltpu.make_async_copy(held.at[n], out_ref.at[0, 0, :, k : k + KMAX], sem.at[n]))
        copies[-1].start()
    for c in copies:
        c.wait()


def kernel(
    slabs, patches, parts,
    r_hbm, l_hbm, f_hbm, b_hbm, margin_ref, out_ref,
    r_v, fac, maps,
    tail_s, head_s, zt_s, zh_s, d_s, u_s,
    tail_r, head_r, zt_r, zh_r, d_r, u_r,
    adj, acc, gt, opd, opu, place, zr,
    load_sem, send_sem, recv_sem,
):
    s = lax.axis_index("slab")
    q = lax.axis_index("patch")
    left = lax.rem(q + patches - 1, patches)
    right = lax.rem(q + 1, patches)
    around = (left, right, q)
    m = fac.shape[-1]
    face = f_hbm.shape[-2]
    cols = r_v.shape[0]
    step = cols // parts
    first_slab, last_slab = s == 0, s == slabs - 1
    inner_low, inner_high = s > 0, s < slabs - 1

    loads = [
        pltpu.make_async_copy(r_hbm.at[0, 0], r_v, load_sem.at[0]),
        pltpu.make_async_copy(l_hbm.at[0, 0], fac, load_sem.at[1]),
        pltpu.make_async_copy(f_hbm.at[0, 0], maps.at[:face], load_sem.at[2]),
        pltpu.make_async_copy(b_hbm.at[0, 0], maps.at[face:], load_sem.at[3]),
    ]
    for c in loads:
        c.start()

    barrier = pltpu.get_barrier_semaphore()

    def greet(slab, patch):
        pl.semaphore_signal(barrier, inc=1, device_id=(slab, patch), device_id_type=MESH)

    greet(s, left)
    greet(s, right)

    @pl.when(inner_low)
    def _():
        for p in around:
            greet(s - 1, p)

    @pl.when(inner_high)
    def _():
        for p in around:
            greet(s + 1, p)

    slot = [0]

    def send(src, dst, slab, patch):
        n = slot[0]
        slot[0] += 1
        return pltpu.make_async_remote_copy(
            src_ref=src, dst_ref=dst, send_sem=send_sem.at[n], recv_sem=recv_sem.at[n],
            device_id=(slab, patch), device_id_type=MESH,
        )

    rows = [pl.ds(c * step, step) for c in range(parts)]
    tail_c = [send(tail_s.at[w], tail_r.at[w], s, right) for w in rows]
    head_c = [send(head_s.at[w], head_r.at[w], s, left) for w in rows]
    low_rows, high_rows = pl.ds(0, face), pl.ds(face, face)
    zd_c = [send(zt_s.at[low_rows], zt_r.at[low_rows], s, right), send(zh_s.at[low_rows], zh_r.at[low_rows], s, left)]
    zu_c = [send(zt_s.at[high_rows], zt_r.at[high_rows], s, right), send(zh_s.at[high_rows], zh_r.at[high_rows], s, left)]
    targets = ((2, left), (1, right), (0, q))
    down_c = [[send(d_s.at[w], d_r.at[j, w], s + 1, p) for j, p in targets] for w in rows]
    up_c = [[send(u_s.at[w], u_r.at[j, w], s - 1, p) for j, p in targets] for w in rows]

    count = margin_ref[0, 0]
    row = lax.broadcasted_iota(jnp.int32, (KMAX, KMAX), 0)
    col = lax.broadcasted_iota(jnp.int32, (KMAX, KMAX), 1)
    hit = (row == KMAX - count + col) & (col < count)
    place[...] = jnp.where(hit, 1.0, 0.0).astype(BF)

    loads[0].wait()
    loads[1].wait()
    first = solve(r_v[...].astype(BF), fac, m)
    tail_s[...] = nn(first[-1].astype(BF), place[...]).astype(BF)
    head_s[...] = first[0].astype(BF)

    pl.semaphore_wait(barrier, 2 + 3 * inner_low.astype(jnp.int32) + 3 * inner_high.astype(jnp.int32))

    for a, b in zip(tail_c, head_c):
        a.start()
        b.start()

    loads[2].wait()
    loads[3].wait()
    for k, part in enumerate(solve(maps[...], fac, m)):
        gt[:, k * KMAX : (k + 1) * KMAX] = part.astype(BF)

    low = fac[:, :face]
    high = fac[m - face :, m - face :]
    k_tail = jnp.concatenate(
        [tn(low[m - KMAX :], fac[m - KMAX :, m - KMAX :]), tn(high, fac[m - face :, m - KMAX :])], axis=0
    )
    k_head = jnp.concatenate([tn(low, fac[:, :KMAX]), tn(high, fac[m - face :, :KMAX])], axis=0)
    zt_s[...] = nn(k_tail.astype(BF), place[...]).astype(BF)
    zh_s[...] = k_head.astype(BF)

    @pl.when(inner_low)
    def _():
        for c in zd_c:
            c.start()

    @pl.when(inner_low & inner_high)
    def _():
        for c in zu_c:
            c.start()

    def send_down(c):
        w = rows[c]
        d_s[w] = acc[w, :face].astype(BF)
        for x in down_c[c]:
            x.start()

    def send_up(c):
        w = rows[c]
        u_s[w] = acc[w, face:].astype(BF)
        for x in up_c[c]:
            x.start()

    for c, w in enumerate(rows):
        tail_c[c].wait_recv()
        head_c[c].wait_recv()
        adj[w, :] = r_v[w, :]
        adj[w, :KMAX] = adj[w, :KMAX] - 0.5 * tail_r[w].astype(F32)
        adj[w, m - KMAX :] = adj[w, m - KMAX :] - 0.5 * nt(head_r[w], place[...])
        acc[w, :face] = nt(adj[w, :].astype(BF), gt[:face])

        @pl.when(first_slab)
        def _():
            send_down(c)

    @pl.when(first_slab)
    def _():
        for c in zu_c:
            c.start()

    acc[:, face:] = nt(adj[...].astype(BF), gt[face:])

    @pl.when(inner_low)
    def _():
        for c in zd_c:
            c.wait_recv()
        zr[low_rows] = nt(zh_r[low_rows], place[...]).astype(BF)
        opd[:face, :] = (-gt[:, :face].astype(F32)).T.astype(BF)
        opd[face : 2 * face, :] = (0.5 * nt(zt_r[low_rows], gt[:, :KMAX])).astype(BF)
        opd[2 * face :, :] = (0.5 * nt(zr[low_rows], gt[:, m - KMAX :])).astype(BF)

    def make_up():
        for c in zu_c:
            c.wait_recv()
        zr[high_rows] = nt(zh_r[high_rows], place[...]).astype(BF)

        @pl.when(inner_low)
        def _():
            opu[:face, :] = (-gt[face:, m - face :].astype(F32)).T.astype(BF)
            opu[face : 2 * face, :] = (0.5 * nt(zt_r[high_rows], gt[face:, :KMAX])).astype(BF)
            opu[2 * face :, :] = (0.5 * nt(zr[high_rows], gt[face:, m - KMAX :])).astype(BF)

    def beside(ref, w):
        return jnp.concatenate([ref[0, w], ref[1, w], ref[2, w]], axis=1)

    @pl.when(inner_low)
    def _():
        for c, w in enumerate(rows):
            for x in down_c[c]:
                x.wait_recv()

            @pl.when(inner_high)
            def _():
                acc[w, :face] += nn(beside(d_r, w), opd[:, :face])
                send_down(c)

            @pl.when(last_slab)
            def _():
                acc[w, face:] += nn(beside(d_r, w), opd[:, face:])
                send_up(c)

        @pl.when(inner_high)
        def _():
            every = pl.ds(0, cols)
            acc[:, face:] += nn(beside(d_r, every), opd[:, face:])

        adj[:, :face] = adj[:, :face] - d_r[0].astype(F32)
        adj[:, :KMAX] = adj[:, :KMAX] + 0.5 * nn(d_r[1], zt_r[low_rows])
        adj[:, m - KMAX :] = adj[:, m - KMAX :] + 0.5 * nn(d_r[2], zr[low_rows])

    @pl.when(inner_high)
    def _():
        make_up()
        for c, w in enumerate(rows):
            for x in up_c[c]:
                x.wait_recv()

            @pl.when(inner_low)
            def _():
                acc[w, face:] += nn(beside(u_r, w), opu[...])
                send_up(c)

            adj[w, m - face :] = adj[w, m - face :] - u_r[0, w].astype(F32)
            adj[w, :KMAX] = adj[w, :KMAX] + 0.5 * nn(u_r[1, w], zt_r[high_rows])
            adj[w, m - KMAX :] = adj[w, m - KMAX :] + 0.5 * nn(u_r[2, w], zr[high_rows])

    out_ref[...] = halfway(adj[...].astype(BF), fac, m)

    for c in tail_c + head_c:
        c.wait_send()

    @pl.when(inner_low)
    def _():
        for c in zd_c:
            c.wait_send()
        for group in up_c:
            for x in group:
                x.wait_send()

    @pl.when(inner_high)
    def _():
        for c in zu_c:
            c.wait_send()
        for group in down_c:
            for x in group:
                x.wait_send()


def on_device(slabs, patches, right_side, inverse_factor, forward_trace, backward_trace, margin):
    cols, m = right_side.shape[2:]
    face = forward_trace.shape[2]
    parts = 4
    copies = 2 * parts + 4 + 6 * parts
    wide = pltpu.VMEM((cols, KMAX), BF)
    square = pltpu.VMEM((2 * face, KMAX), BF)
    thin = pltpu.VMEM((cols, face), BF)
    three = pltpu.VMEM((3, cols, face), BF)
    hbm = pl.BlockSpec(memory_space=pltpu.HBM)
    half = pl.pallas_call(
        functools.partial(kernel, slabs, patches, parts),
        out_shape=jax.ShapeDtypeStruct((cols, m), BF),
        in_specs=[hbm, hbm, hbm, hbm, pl.BlockSpec(memory_space=pltpu.SMEM)],
        out_specs=pl.BlockSpec(memory_space=pltpu.VMEM),
        scratch_shapes=[
            pltpu.VMEM((cols, m), F32),
            pltpu.VMEM((m, m), BF),
            pltpu.VMEM((2 * face, m), BF),
            wide, wide, square, square, thin, thin,
            wide, wide, square, square, three, three,
            pltpu.VMEM((cols, m), F32),
            pltpu.VMEM((cols, 2 * face), F32),
            pltpu.VMEM((2 * face, m), BF),
            pltpu.VMEM((3 * face, 2 * face), BF),
            pltpu.VMEM((3 * face, face), BF),
            pltpu.VMEM((KMAX, KMAX), BF),
            square,
            pltpu.SemaphoreType.DMA((4,)),
            pltpu.SemaphoreType.DMA((copies,)),
            pltpu.SemaphoreType.DMA((copies,)),
        ],
        compiler_params=pltpu.CompilerParams(collective_id=0, has_side_effects=True),
        name="sweeps",
    )(right_side, inverse_factor, forward_trace, backward_trace, margin)
    return pl.pallas_call(
        finish,
        out_shape=jax.ShapeDtypeStruct(right_side.shape, F32),
        in_specs=[pl.BlockSpec(memory_space=pltpu.VMEM)] * 2,
        out_specs=hbm,
        scratch_shapes=[pltpu.VMEM((m // KMAX, cols, KMAX), F32), pltpu.SemaphoreType.DMA((m // KMAX,))],
        compiler_params=pltpu.CompilerParams(vmem_limit_bytes=16 << 20),
        name="finish",
    )(half, inverse_factor)


def solution(mesh):
    four = P("slab", "patch", None, None)
    return jax.shard_map(
        functools.partial(on_device, mesh.shape["slab"], mesh.shape["patch"]),
        mesh=mesh,
        in_specs=(four, four, four, four, P("slab", "patch")),
        out_specs=four,
        check_vma=False,
    )
```
